32 devices in a mesh: seq: 4 (over z), shard: 8 (over y, x, core).
Axes of the slice: x: 2, y: 2, z: 4, core: 2. Of those that a mesh axis runs over, the one named last changes fastest.
Arguments:
- tokens: bfloat16 [2, 8, 2048, 768], P(None, 'shard', 'seq'), may hold values from -6 to 6
- lengths: int32 [8, 2], P('shard'), may hold values from 512 to 2048, as said below
- w_qkv: bfloat16 [768, 2304], P('shard'), may hold values from -0.21875 to 0.21875
- b_query: bfloat16 [768], P('shard'), may hold values from -3 to 3
- b_value: bfloat16 [768], P('shard'), may hold values from -3 to 3
- w_out: bfloat16 [768, 768], P('shard'), may hold values from -6 to 6
- b_out: bfloat16 [768], P('shard'), may hold values from -3 to 3
- gain_one: bfloat16 [768], P('shard'), may hold values from 0.5 to 1.5
- shift_one: bfloat16 [768], P('shard'), may hold values from -3 to 3
- w_up: bfloat16 [768, 3072], P('shard'), may hold values from -0.21875 to 0.21875
- b_up: bfloat16 [3072], P('shard'), may hold values from -3 to 3
- w_down: bfloat16 [3072, 768], P('shard'), may hold values from -0.109375 to 0.109375
- b_down: bfloat16 [768], P('shard'), may hold values from -3 to 3
- gain_two: bfloat16 [768], P('shard'), may hold values from 0.5 to 1.5
- shift_two: bfloat16 [768], P('shard'), may hold values from -3 to 3
- cotangent: bfloat16 [2, 8, 2048, 768], P(None, 'shard', 'seq'), may hold values from -6 to 6
Outputs:
- layer_out: bfloat16 [2, 8, 2048, 768], P(None, 'shard', 'seq')
- input_grad: bfloat16 [2, 8, 2048, 768], P(None, 'shard', 'seq')
- grad_w_qkv: float32 [768, 2304], P('shard')
- grad_b_query: float32 [768], P('shard')
- grad_b_value: float32 [768], P('shard')
- grad_w_out: float32 [768, 768], P('shard')
- grad_b_out: float32 [768], P('shard')
- grad_gain_one: float32 [768], P('shard')
- grad_shift_one: float32 [768], P('shard')
- grad_w_up: float32 [768, 3072], P('shard')
- grad_b_up: float32 [3072], P('shard')
- grad_w_down: float32 [3072, 768], P('shard')
- grad_b_down: float32 [768], P('shard')
- grad_gain_two: float32 [768], P('shard')
- grad_shift_two: float32 [768], P('shard')
The draws below stay inside these ranges and needn't reach their ends.
Inputs may be any that keep to these rules, and one draw needn't show every extreme that they name: `lengths`: each group's sequence in each micro-batch has this many valid tokens at the start of its 2048 slots; some entry equals 2048.
All inputs are finite; a program needn't handle non-finite values.
Results may differ from the reference program's by a relative error of at most 0.015.
Values may be sent and summed in bfloat16 or wider, within the bound.
A program may use at most 192 MiB of HBM per device.

```python
import math
import jax
import jax.numpy as jnp
from jax import lax

D = 768
H = 12
DH = 64
FF = 3072
SEQ = 2048
MB = 2
GROUPS = 8


def draw_lengths(key, part):
    first, second = jax.random.split(jax.random.fold_in(key, 17))
    values = jax.random.randint(first, (GROUPS * MB,), SEQ // 4, SEQ + 1, dtype=jnp.int32)
    chosen = jax.random.randint(second, (), 0, GROUPS * MB, dtype=jnp.int32)
    filled = jnp.where(jnp.arange(GROUPS * MB, dtype=jnp.int32) == chosen, SEQ, values)
    return filled.reshape(GROUPS, MB).astype(jnp.int32)


def block_scale(key, shape, shards, smallest, largest):
    def one(position, parts):
        heights = jax.random.uniform(jax.random.fold_in(jax.random.fold_in(key, 6), position), (parts,), jnp.float32, smallest / len(shards), largest / len(shards))
        return jnp.repeat(jnp.exp(heights), shape[position] // parts).reshape((-1,) + (1,) * (len(shape) - position - 1))

    factor_of = one(*shards[0])
    for cut in shards[1:]:
        factor_of = factor_of * one(*cut)
    return factor_of


def bell_draw(stream_key, extent, deviation, bound, cuts=(), kind=jnp.bfloat16):
    gain = block_scale(stream_key, extent, cuts, -0.22, 0.18) if cuts else 1.0
    values = jax.random.normal(stream_key, extent, jnp.float32) * deviation * gain
    return jnp.minimum(jnp.maximum(values, -bound), bound).astype(kind)


def setup_inputs(seed: int = 0) -> dict:
    key_list = jax.random.split(jax.random.key(seed), 17)
    tokens = bell_draw(key_list[0], (MB, GROUPS, SEQ, D), 1.0, 6.0, ((1, 8), (2, 4)))
    lengths = draw_lengths(jax.random.fold_in(key_list[16], 71), 0)
    w_qkv = bell_draw(key_list[2], (D, 3 * D), D ** -0.5, 0.21875, ((0, 8),))
    b_query = bell_draw(key_list[3], (D,), 0.5, 3.0, ((0, 8),))
    b_value = bell_draw(key_list[4], (D,), 0.5, 3.0, ((0, 8),))
    w_out = bell_draw(key_list[5], (D, D), (max(1, 2 * D // SEQ)) ** -0.5, 6.0, ((0, 8),))
    b_out = bell_draw(key_list[6], (D,), 0.5, 3.0, ((0, 8),))
    gain_one = jnp.clip(1.0 + 0.1 * jax.random.normal(key_list[7], (D,), jnp.float32), 0.5, 1.5).astype(jnp.bfloat16)
    shift_one = bell_draw(key_list[8], (D,), 0.5, 3.0, ((0, 8),))
    w_up = bell_draw(key_list[9], (D, FF), D ** -0.5, 0.21875, ((0, 8),))
    b_up = bell_draw(key_list[10], (FF,), 0.5, 3.0, ((0, 8),))
    w_down = bell_draw(key_list[11], (FF, D), FF ** -0.5, 0.109375, ((0, 8),))
    b_down = bell_draw(key_list[12], (D,), 0.5, 3.0, ((0, 8),))
    gain_two = jnp.clip(1.0 + 0.1 * jax.random.normal(key_list[13], (D,), jnp.float32), 0.5, 1.5).astype(jnp.bfloat16)
    shift_two = bell_draw(key_list[14], (D,), 0.5, 3.0, ((0, 8),))
    cotangent = bell_draw(key_list[15], (MB, GROUPS, SEQ, D), 1.0, 6.0, ((1, 8), (2, 4)))
    return {"tokens": tokens, "lengths": lengths, "w_qkv": w_qkv, "b_query": b_query, "b_value": b_value, "w_out": w_out, "b_out": b_out, "gain_one": gain_one, "shift_one": shift_one, "w_up": w_up, "b_up": b_up, "w_down": w_down, "b_down": b_down, "gain_two": gain_two, "shift_two": shift_two, "cotangent": cotangent}


norm_eps = 1e-06

@jax.custom_vjp
def low(v):
    return lax.optimization_barrier(v.astype(jnp.bfloat16)).astype(jnp.float32)

@jax.custom_vjp
def low_back(v):
    return v

def low_keep(v):
    return (low(v), None)

def low_pass(kept, grad):
    return (grad,)

def back_keep(v):
    return (v, None)

def back_low(kept, grad):
    return (low(grad),)
low.defvjp(low_keep, low_pass)
low_back.defvjp(back_keep, back_low)

def layer_norm(inputs, scales, shifts):
    centre = lax.optimization_barrier(jnp.mean(inputs, axis=-1, keepdims=True))
    centred = inputs - centre
    spread = lax.optimization_barrier(jnp.mean(centred * centred, axis=-1, keepdims=True))
    return centred * lax.rsqrt(spread + norm_eps) * scales + shifts

def product(left, right):
    return jnp.dot(left, right, precision=lax.Precision.HIGHEST, preferred_element_type=jnp.float32)

def sequence_layer(parameters, inputs, seq_length):
    qkv_matrix, query_bias, value_bias, out_matrix, out_bias, gain_first, shift_first, up_matrix, up_bias, down_matrix, down_bias, gain_second, shift_second = parameters
    bias_all = jnp.concatenate([query_bias, jnp.zeros_like(query_bias), value_bias])
    projected = low_back(low(product(inputs, qkv_matrix) + bias_all))
    split_heads = projected.reshape(SEQ, 3, H, DH)
    queries = split_heads[:, 0]
    key_rows = split_heads[:, 1]
    value_rows = split_heads[:, 2]
    key_valid = jnp.arange(SEQ, dtype=jnp.int32) < seq_length
    scaling = 1.0 / math.sqrt(DH)
    block_rows = min(512, SEQ)

    def attend(q_block):
        raw_scores = jnp.einsum('qhd,khd->hqk', q_block, key_rows, precision=lax.Precision.HIGHEST)
        scores = low_back(raw_scores * scaling)
        masked = jnp.where(key_valid[None, None, :], scores, -1e+30)
        probs = jax.nn.softmax(masked, axis=-1)
        return jnp.einsum('hqk,khd->qhd', low(probs), value_rows, precision=lax.Precision.HIGHEST)
    context = lax.map(jax.checkpoint(attend), queries.reshape(SEQ // block_rows, block_rows, H, DH))
    context = low_back(low(context.reshape(SEQ, D)))
    attn_branch = low_back(product(context, out_matrix) + out_bias)
    hidden_one = layer_norm(inputs + attn_branch, gain_first, shift_first)
    up_proj = low_back(product(low(hidden_one), up_matrix) + up_bias)
    activated = low(jax.nn.gelu(up_proj, approximate=False))
    down_branch = low_back(product(activated, down_matrix) + down_bias)
    return layer_norm(hidden_one + down_branch, gain_second, shift_second)

def reference(tokens, lengths, w_qkv, b_query, b_value, w_out, b_out, gain_one, shift_one, w_up, b_up, w_down, b_down, gain_two, shift_two, cotangent):
    parameters = (w_qkv.astype(jnp.float32), b_query.astype(jnp.float32), b_value.astype(jnp.float32), w_out.astype(jnp.float32), b_out.astype(jnp.float32), gain_one.astype(jnp.float32), shift_one.astype(jnp.float32), w_up.astype(jnp.float32), b_up.astype(jnp.float32), w_down.astype(jnp.float32), b_down.astype(jnp.float32), gain_two.astype(jnp.float32), shift_two.astype(jnp.float32))
    flat_tokens = tokens.astype(jnp.float32).reshape(MB * GROUPS, SEQ, D)
    flat_lengths = jnp.transpose(lengths).reshape(MB * GROUPS).astype(jnp.int32)
    checked = jax.checkpoint(sequence_layer)

    def forward(parameters, flat_tokens):
        return lax.map(lambda pair: checked(parameters, pair[0], pair[1]), (flat_tokens, flat_lengths))
    outputs, pullback = jax.vjp(forward, parameters, flat_tokens)
    row_valid = (jnp.arange(SEQ, dtype=jnp.int32)[None, :] < flat_lengths[:, None]).astype(jnp.float32)
    seed_grad = cotangent.astype(jnp.float32).reshape(MB * GROUPS, SEQ, D) * row_valid[:, :, None]
    grad_params, token_grads = pullback(seed_grad)
    return (outputs.reshape(MB, GROUPS, SEQ, D).astype(jnp.bfloat16), token_grads.reshape(MB, GROUPS, SEQ, D).astype(jnp.bfloat16), grad_params[0], grad_params[1], grad_params[2], grad_params[3], grad_params[4], grad_params[5], grad_params[6], grad_params[7], grad_params[8], grad_params[9], grad_params[10], grad_params[11], grad_params[12])
```

```python
import functools
import math

import jax
import jax.numpy as jnp
from jax import lax
from jax.sharding import PartitionSpec as P
from jax.experimental import pallas as pl
from jax.experimental.pallas import tpu as pltpu

LANES = 128
f32 = jnp.float32
bf16 = jnp.bfloat16


def dot_nt(a, b):
    return lax.dot_general(a, b, (((1,), (1,)), ((), ())), preferred_element_type=f32)


def dot_tn(a, b):
    return lax.dot_general(a, b, (((0,), (0,)), ((), ())), preferred_element_type=f32)


def dot_nn(a, b):
    return jnp.dot(a, b, preferred_element_type=f32)


def keys_of_head(keys, length, head):
    shape = keys.shape
    lane = lax.broadcasted_iota(jnp.int32, shape, 1)
    row = lax.broadcasted_iota(jnp.int32, shape, 0)
    half = LANES // 2
    spare = half * (1 - head)
    bias = jnp.where(row < length, 0.0, -1e30).astype(f32)
    kept = jnp.where((lane // half) == head, keys.astype(f32), 0.0)
    return jnp.where(lane == spare, bias, kept).astype(bf16)


def rows_of_head(rows, head, spare_value):
    lane = lax.broadcasted_iota(jnp.int32, rows.shape, 1)
    half = LANES // 2
    kept = jnp.where((lane // half) == head, rows.astype(f32), 0.0)
    if spare_value:
        kept = jnp.where(lane == half * (1 - head), spare_value, kept)
    return kept.astype(bf16)


def attn_fwd_kernel(len_ref, order_ref, q_ref, k_ref, v_ref, o_ref, lse_ref, key_scr, val_scr, s_scr, *, chunk):
    slots = k_ref.shape[0]
    rows = q_ref.shape[0]

    @pl.when(pl.program_id(1) == 0)
    def _():
        for head in range(2):
            key_scr[head] = keys_of_head(k_ref[...], len_ref[0], head)
        val_scr[:, :LANES] = v_ref[...]
        val_scr[:, LANES:] = jnp.ones((slots, LANES), bf16)

    queries = q_ref[...]
    lane = lax.broadcasted_iota(jnp.int32, (rows, LANES), 1)
    result = None
    for head in range(2):
        qa = rows_of_head(queries, head, 1.0)
        top = None
        for start in range(0, slots, chunk):
            s = dot_nt(qa, key_scr[head, start : start + chunk, :])
            s_scr[head, :, start : start + chunk] = s
            for part in range(0, chunk, LANES):
                piece = s[:, part : part + LANES]
                top = piece if top is None else jnp.maximum(top, piece)
        top = jnp.max(top, axis=1, keepdims=True)
        acc = None
        for start in range(0, slots, chunk):
            p = jnp.exp(s_scr[head, :, start : start + chunk] - top).astype(bf16)
            term = dot_nn(p, val_scr[start : start + chunk, :])
            acc = term if acc is None else acc + term
        total = acc[:, LANES:]
        out = acc[:, :LANES] / total
        lse = jnp.transpose(jnp.broadcast_to(top, (rows, LANES)) + jnp.log(total))
        lse_ref[0, head : head + 1, :] = lse[0:1, :]
        result = out if result is None else jnp.where(lane < LANES // 2, result, out)
    o_ref[...] = result.astype(bf16)


def attention_forward(qkv, length, order, rows, chunk=512):
    slots, width = qkv.shape
    pairs = width // (3 * LANES)
    blocks = order.shape[0]
    return pl.pallas_call(
        functools.partial(attn_fwd_kernel, chunk=chunk),
        out_shape=(
            jax.ShapeDtypeStruct((blocks * rows, pairs * LANES), bf16),
            jax.ShapeDtypeStruct((pairs, 8, blocks * rows), f32),
        ),
        grid_spec=pltpu.PrefetchScalarGridSpec(
            num_scalar_prefetch=2,
            grid=(pairs, blocks),
            in_specs=[
                pl.BlockSpec((rows, LANES), lambda g, i, n, o: (o[i], g)),
                pl.BlockSpec((slots, LANES), lambda g, i, n, o: (0, pairs + g)),
                pl.BlockSpec((slots, LANES), lambda g, i, n, o: (0, 2 * pairs + g)),
            ],
            out_specs=[
                pl.BlockSpec((rows, LANES), lambda g, i, n, o: (i, g)),
                pl.BlockSpec((1, 8, rows), lambda g, i, n, o: (g, 0, i)),
            ],
            scratch_shapes=[
                pltpu.VMEM((2, slots, LANES), bf16),
                pltpu.VMEM((slots, 2 * LANES), bf16),
                pltpu.VMEM((2, rows, slots), f32),
            ],
        ),
        compiler_params=pltpu.CompilerParams(
            dimension_semantics=("arbitrary", "arbitrary"), vmem_limit_bytes=48 << 20
        ),
        cost_estimate=pl.CostEstimate(
            flops=16 * blocks * rows * slots * pairs * LANES,
            transcendentals=2 * pairs * slots * blocks * rows,
            bytes_accessed=2 * slots * width * 2,
        ),
        name="attn_fwd",
    )(length, order, qkv, qkv, qkv)


def attn_bwd_kernel(
    len_ref, order_ref, q_ref, k_ref, v_ref, o_ref, do_ref, lse_ref,
    dq_ref, dk_ref, dv_ref, key_scr, dk_scr, dv_scr, *, chunk, scaling,
):
    slots = k_ref.shape[0]
    step = pl.program_id(1)

    @pl.when(step == 0)
    def _():
        for head in range(2):
            key_scr[head] = keys_of_head(k_ref[...], len_ref[0], head)
        dk_scr[...] = jnp.zeros_like(dk_scr)
        dv_scr[...] = jnp.zeros_like(dv_scr)

    queries = q_ref[...]
    grads = do_ref[...]
    prod = grads.astype(f32) * o_ref[...].astype(f32)
    lane8 = lax.broadcasted_iota(jnp.int32, (8, LANES), 1)
    dq = None
    for head in range(2):
        pick = jnp.where((lane8 // (LANES // 2)) == head, 1.0, 0.0).astype(f32)
        delta = lax.dot_general(
            pick, prod, (((1,), (1,)), ((), ())),
            precision=lax.Precision.HIGHEST, preferred_element_type=f32,
        )[0:1, :]
        lse = lse_ref[0, head : head + 1, :]
        qx = rows_of_head(queries, head, 1.0)
        qa = rows_of_head(queries, head, 0.0)
        da = rows_of_head(grads, head, 0.0)
        for start in range(0, slots, chunk):
            here = slice(start, start + chunk)
            keys = key_scr[head, here, :]
            p = jnp.exp(dot_nt(keys, qx) - lse)
            ds = (p * (dot_nt(v_ref[here, :], da) - delta)).astype(bf16)
            dv_scr[here, :] += dot_nn(p.astype(bf16), da)
            dk_scr[here, :] += dot_nn(ds, qa)
            term = dot_tn(ds, keys)
            dq = term if dq is None else dq + term
    dq_ref[...] = (dq * scaling).astype(bf16)

    @pl.when(step == pl.num_programs(1) - 1)
    def _():
        dk_ref[...] = dk_scr[...].astype(bf16)
        dv_ref[...] = dv_scr[...].astype(bf16)


def attention_backward(qkv, length, order, context, grad, lse, scaling, rows, chunk=1024):
    slots, width = qkv.shape
    pairs = width // (3 * LANES)
    shape = jax.ShapeDtypeStruct((slots, pairs * LANES), bf16)
    return pl.pallas_call(
        functools.partial(attn_bwd_kernel, chunk=chunk, scaling=scaling),
        out_shape=(shape, shape, shape),
        grid_spec=pltpu.PrefetchScalarGridSpec(
            num_scalar_prefetch=2,
            grid=(pairs, slots // rows),
            in_specs=[
                pl.BlockSpec((rows, LANES), lambda g, i, n, o: (o[i], g)),
                pl.BlockSpec((slots, LANES), lambda g, i, n, o: (0, pairs + g)),
                pl.BlockSpec((slots, LANES), lambda g, i, n, o: (0, 2 * pairs + g)),
                pl.BlockSpec((rows, LANES), lambda g, i, n, o: (i, g)),
                pl.BlockSpec((rows, LANES), lambda g, i, n, o: (i, g)),
                pl.BlockSpec((1, 8, rows), lambda g, i, n, o: (g, 0, i)),
            ],
            out_specs=[
                pl.BlockSpec((rows, LANES), lambda g, i, n, o: (o[i], g)),
                pl.BlockSpec((slots, LANES), lambda g, i, n, o: (0, g)),
                pl.BlockSpec((slots, LANES), lambda g, i, n, o: (0, g)),
            ],
            scratch_shapes=[
                pltpu.VMEM((2, slots, LANES), bf16),
                pltpu.VMEM((slots, LANES), f32),
                pltpu.VMEM((slots, LANES), f32),
            ],
        ),
        compiler_params=pltpu.CompilerParams(
            dimension_semantics=("arbitrary", "arbitrary"), vmem_limit_bytes=48 << 20
        ),
        cost_estimate=pl.CostEstimate(
            flops=40 * slots * slots * pairs * LANES,
            transcendentals=2 * pairs * slots * slots,
            bytes_accessed=4 * slots * width * 2,
        ),
        name="attn_bwd",
    )(length, order, qkv, qkv, qkv, context, grad, lse)


H = 12
norm_eps = 1e-06
ERF_P = 0.32
ERF_C = (
    0.18140208045914907,
    0.16781523017336925,
    0.2520604501706694,
    -0.13396961774602328,
    0.7456596101028902,
    -0.724323250347485,
    0.6843514662938643,
    -0.17299593051459605,
)


def gelu_parts(u):
    t = 1.0 / (1.0 + (ERF_P / math.sqrt(2.0)) * jnp.abs(u))
    bell = jnp.exp(-0.5 * u * u)
    poly = ERF_C[-1]
    for coefficient in ERF_C[-2::-1]:
        poly = poly * t + coefficient
    tail = 0.5 * poly * t * bell
    phi = jnp.where(u >= 0, 1.0 - tail, tail)
    return u * phi, phi + u * bell * (1.0 / math.sqrt(2.0 * math.pi))


def norm_parts(rows):
    centred = rows - jnp.mean(rows, axis=-1, keepdims=True)
    scale = lax.rsqrt(jnp.mean(centred * centred, axis=-1, keepdims=True) + norm_eps)
    return centred * scale, scale


def norm_back(grad, normed, scale, gain):
    e = grad * gain
    return scale * (
        e
        - jnp.mean(e, axis=-1, keepdims=True)
        - normed * jnp.mean(e * normed, axis=-1, keepdims=True)
    )


class Lines:
    def __init__(self):
        self.n_seq = lax.axis_size("seq")
        self.n_shard = lax.axis_size("shard")
        self.z = lax.axis_index("seq")
        self.shard = lax.axis_index("shard")
        self.core = lax.rem(self.shard, 2)

    def device(self, z, shard):
        return z * self.n_shard + shard

    def towards(self, step):
        pairs = []
        for z in range(self.n_seq):
            for shard in range(self.n_shard):
                p = (z + step) % self.n_seq
                there = self.device(2 * (p // 2) + shard % 2, 2 * (shard // 2) + p % 2)
                pairs.append((self.device(z, shard), there))
        return pairs

    def send(self, piece, step):
        return lax.ppermute(piece, ("seq", "shard"), self.towards(step))

    def send_back(self, piece, step):
        return lax.ppermute(piece, ("seq", "shard"), [(b, a) for a, b in self.towards(step)])

    def swap(self, piece):
        return lax.ppermute(piece, "shard", [(k, k ^ 1) for k in range(self.n_shard)])

    def target(self, step):
        return lax.rem(self.z + step, self.n_seq)

    def source(self, step, core):
        return lax.rem(2 * (self.z // 2) + core - step + self.n_seq, self.n_seq)


def put(whole, piece, *starts):
    return lax.dynamic_update_slice(whole, piece, starts)


def layer(
    tokens,
    lengths,
    w_qkv,
    b_query,
    b_value,
    w_out,
    b_out,
    gain_one,
    shift_one,
    w_up,
    b_up,
    w_down,
    b_down,
    gain_two,
    shift_two,
    cotangent,
):
    lines = Lines()
    micro, _, rows, width = tokens.shape
    n_seq, n_shard, core = lines.n_seq, lines.n_shard, lines.core
    assert micro * 2 == n_seq
    half_rows = rows // 2
    half = width // 2
    hidden = w_up.shape[1]
    slots = rows * n_seq
    scaling = 1.0 / math.sqrt(width // H)
    parity = [[k for k in range(n_shard) if k % 2 == c] for c in range(2)]

    x_home = tokens[:, 0].reshape(n_seq, half_rows, width)
    x_seq = jnp.zeros((slots, width), bf16)
    for step in range(n_seq):
        piece = lines.send(
            lax.dynamic_index_in_dim(x_home, lines.target(step), 0, keepdims=False), step
        )
        other = lines.swap(piece)
        own_at = lines.source(step, core) * rows + core * half_rows
        other_at = lines.source(step, 1 - core) * rows + (1 - core) * half_rows
        x_seq = put(x_seq, piece, own_at, 0)
        x_seq = put(x_seq, other, other_at, 0)
    there = lines.swap(lengths)
    length = jnp.where(lax.rem(lines.z, 2) == core, lengths, there)
    length = lax.dynamic_index_in_dim(length[0], lines.z // 2, 0)

    small = jnp.concatenate(
        [b_query, b_value, b_out, gain_one, shift_one, b_down, gain_two, shift_two, b_up]
    )
    small_rows = -(-small.shape[0] // (3 * half))
    small = jnp.pad(small, (0, small_rows * 3 * half - small.shape[0]))
    shard_rows = w_qkv.shape[0]
    extra = -(-small_rows // 16) * 16
    columns = w_qkv.reshape(shard_rows, 3, 2, half)
    small = jnp.pad(small.reshape(small_rows, 3 * half), ((0, extra - small_rows), (0, 0)))

    def package(which):
        picked = lax.dynamic_index_in_dim(columns, which, 2, keepdims=False)
        return jnp.concatenate([picked.reshape(shard_rows, 3 * half), small])

    mine, theirs = package(core), lines.swap(package(1 - core))
    both = jnp.stack(
        [jnp.where(core == 0, mine, theirs), jnp.where(core == 0, theirs, mine)]
    )
    everyone = lax.all_gather(both, "shard", axis_index_groups=parity, axis=0, tiled=True)
    qkv_matrix = everyone[:, :shard_rows].reshape(width, 3 * half)
    vectors = everyone[:, shard_rows : shard_rows + small_rows].reshape(n_shard, -1)
    vectors = vectors.astype(f32)
    per = width // n_shard

    def vector(place):
        return vectors[:, place * per : (place + 1) * per].reshape(width)

    query_bias, value_bias, out_bias, gain_first, shift_first, down_bias, gain_second, shift_second = (
        vector(place) for place in range(8)
    )
    up_bias = vectors[:, 8 * per : 8 * per + hidden // n_shard].reshape(hidden)

    out_matrix = lax.all_gather(w_out, "shard", axis=0, tiled=True)
    up_matrix = lax.all_gather(w_up, "shard", axis=0, tiled=True)
    down_matrix = lax.all_gather(w_down, "shard", axis=0, tiled=True)

    head_bias = jnp.concatenate(
        [
            lax.dynamic_slice(query_bias, (core * half,), (half,)),
            jnp.zeros((half,), f32),
            lax.dynamic_slice(value_bias, (core * half,), (half,)),
        ]
    )
    head_scale = jnp.where(jnp.arange(3 * half) < half, scaling, 1.0).astype(f32)
    qkv = (
        (dot_nn(x_seq, qkv_matrix) + head_bias).astype(bf16).astype(f32) * head_scale
    ).astype(bf16)
    order = jnp.stack([lines.source(step, core) for step in range(n_seq)]).astype(jnp.int32)
    blocks, parts, log_totals = [], [], []
    for first in range(0, n_seq, 2):
        block, log_total = attention_forward(qkv, length, order[first : first + 2], rows)
        log_totals.append(log_total)
        blocks.append(block)
        for step in (first, first + 1):
            parts.append(lines.send_back(block[(step - first) * rows :][:rows], step))
    context_seq = jnp.concatenate(blocks)
    log_total = jnp.concatenate(log_totals, axis=2)
    parts = jnp.stack(parts + parts)
    parts = lax.dynamic_slice_in_dim(parts, lax.rem(n_seq - lines.z, n_seq), n_seq)
    parts = parts.reshape(micro, 2, rows, half)
    left, right = (parts[:, k].reshape(micro * rows, half) for k in range(2))

    inputs = tokens[:, 0].reshape(micro * rows, width).astype(f32)
    positions = lines.z * rows + jnp.arange(rows, dtype=jnp.int32)
    row_valid = (positions[None, :] < lengths[0][:, None]).reshape(micro * rows, 1)
    residual_one = inputs + dot_nn(left, out_matrix[:half]) + dot_nn(right, out_matrix[half:]) + out_bias
    normed_one, scale_one = norm_parts(residual_one)
    hidden_one = normed_one * gain_first + shift_first
    hidden_low = hidden_one.astype(bf16)
    up_proj = dot_nn(hidden_low, up_matrix) + up_bias
    activated, slope = gelu_parts(up_proj)
    activated, slope = lax.optimization_barrier((activated.astype(bf16), slope))
    residual_two = hidden_one + dot_nn(activated, down_matrix) + down_bias
    normed_two, scale_two = norm_parts(residual_two)
    layer_out = (normed_two * gain_second + shift_second).astype(bf16)

    out_grad = jnp.where(
        row_valid, cotangent[:, 0].reshape(micro * rows, width).astype(f32), 0.0
    )
    grad_two = norm_back(out_grad, normed_two, scale_two, gain_second)
    down_grad = grad_two.astype(bf16)
    up_grad = (dot_nt(down_grad, down_matrix) * slope).astype(bf16)
    grad_hidden = grad_two + dot_nt(up_grad, up_matrix)
    grad_one = norm_back(grad_hidden, normed_one, scale_one, gain_first)
    attn_grad = grad_one.astype(bf16)
    context_grad = dot_nt(attn_grad, out_matrix).astype(bf16)

    arrived = []
    for step in range(n_seq):
        target = lines.target(step)
        block = lax.dynamic_slice(
            context_grad, ((target // 2) * rows, lax.rem(target, 2) * half), (rows, half)
        )
        arrived.append(lines.send(block, step))
    context_grad_seq = jnp.concatenate(arrived)

    def by_shard(matrix):
        return matrix.reshape((n_shard, -1) + matrix.shape[1:])

    def column_sum(values):
        return jnp.sum(values.astype(f32), axis=0)

    small_grads = [
        column_sum(attn_grad),
        column_sum(grad_hidden * normed_one),
        column_sum(grad_hidden),
        column_sum(down_grad),
        column_sum(out_grad * normed_two),
        column_sum(out_grad),
        column_sum(up_grad),
    ]
    small_grads = jnp.concatenate([by_shard(g) for g in small_grads], axis=1)
    tail_rows = -(-small_grads.shape[1] // width)
    tail_rows = -(-tail_rows // 16) * 16
    small_grads = jnp.pad(
        small_grads, ((0, 0), (0, tail_rows * width - small_grads.shape[1]))
    ).reshape(n_shard, tail_rows, width)
    grad_up = by_shard(dot_tn(hidden_low, up_grad))
    grad_down = by_shard(dot_tn(activated, down_grad))
    grad_out = dot_tn(left, attn_grad)
    grad_out = by_shard(jnp.concatenate([grad_out, dot_tn(right, attn_grad)]))
    bundle = jnp.concatenate(
        [grad_up[..., k * width :][..., :width] for k in range(hidden // width)]
        + [grad_down, grad_out, small_grads],
        axis=1,
    ).astype(bf16)

    def reduce_shard(pieces, groups=None):
        flat = pieces.reshape((-1,) + pieces.shape[2:])
        return lax.psum_scatter(
            flat, "shard", scatter_dimension=0, axis_index_groups=groups, tiled=True
        )

    context_grad_seq, bundle = lax.optimization_barrier((context_grad_seq, bundle))
    bundle = reduce_shard(bundle)

    grad_query, grad_key, grad_value = attention_backward(
        qkv, length, order, context_seq, context_grad_seq, log_total, scaling, rows
    )
    qkv_grad = jnp.concatenate([grad_query, grad_key, grad_value], axis=1)
    by_half = qkv_grad.reshape(n_seq, 2, half_rows, 3 * half)

    def half_of_rows(which):
        picked = lax.dynamic_index_in_dim(by_half, which, 1, keepdims=False)
        return dot_nt(picked.reshape(-1, 3 * half), qkv_matrix)

    given = half_of_rows(1 - core).astype(bf16)
    given = lines.swap(given)
    joined = (half_of_rows(core) + given.astype(f32)).astype(bf16)
    joined = joined.reshape(n_seq, half_rows, width)
    back = jnp.zeros((n_seq, half_rows, width), bf16)
    for step in range(n_seq):
        block = lax.dynamic_index_in_dim(joined, lines.source(step, core), 0)
        block = lines.send_back(block, step)
        back = put(back, block, lines.target(step), 0, 0)
    input_grad = (grad_one + back.reshape(micro * rows, width).astype(f32)).astype(bf16)

    pair_rows = 2 * shard_rows
    groups = n_shard // 2
    bias_rows = jnp.pad(
        jnp.broadcast_to(column_sum(qkv_grad), (groups, 1, 3 * half)), ((0, 0), (0, 15), (0, 0))
    )
    grad_qkv = dot_tn(x_seq, qkv_grad).reshape(groups, pair_rows, 3 * half)
    grad_qkv = jnp.concatenate([grad_qkv, bias_rows], axis=1).astype(bf16)
    grad_qkv = reduce_shard(grad_qkv, parity)
    grad_qkv, bundle = lax.psum((grad_qkv, bundle), "seq")
    bundle = bundle.astype(f32)
    bias_row = grad_qkv[pair_rows : pair_rows + 16]
    own = lax.dynamic_slice(grad_qkv, (core * shard_rows, 0), (shard_rows, 3 * half))
    other = lax.dynamic_slice(grad_qkv, ((1 - core) * shard_rows, 0), (shard_rows, 3 * half))
    mine = jnp.concatenate([own, bias_row])
    theirs = lines.swap(jnp.concatenate([other, bias_row]))
    halves = jnp.stack(
        [jnp.where(core == 0, mine, theirs), jnp.where(core == 0, theirs, mine)], axis=1
    ).astype(f32)
    halves = halves.reshape(-1, 2, 3, half).transpose(0, 2, 1, 3).reshape(-1, 3 * width)
    grad_w_qkv = halves[:shard_rows]
    bias_grad = halves[shard_rows]
    mine_at = lines.shard * per
    grad_b_query = lax.dynamic_slice(bias_grad, (mine_at,), (per,))
    grad_b_value = lax.dynamic_slice(bias_grad, (2 * width + mine_at,), (per,))

    edges = [shard_rows * k for k in range(hidden // width + 1)]
    grad_up = jnp.concatenate(
        [bundle[a:b] for a, b in zip(edges, edges[1:])], axis=1
    )
    down_at = edges[-1]
    out_at = down_at + hidden // n_shard
    tail_at = out_at + shard_rows
    tail = bundle[tail_at:].reshape(-1)
    grad_b_out, grad_gain_one, grad_shift_one, grad_b_down, grad_gain_two, grad_shift_two = (
        tail[place * per : (place + 1) * per] for place in range(6)
    )
    grad_b_up = tail[6 * per : 6 * per + hidden // n_shard]
    return (
        layer_out.reshape(tokens.shape),
        input_grad.reshape(tokens.shape),
        grad_w_qkv,
        grad_b_query,
        grad_b_value,
        bundle[out_at:tail_at],
        grad_b_out,
        grad_gain_one,
        grad_shift_one,
        grad_up,
        grad_b_up,
        bundle[down_at:out_at],
        grad_b_down,
        grad_gain_two,
        grad_shift_two,
    )


def solution(mesh):
    placed = (
        P(None, "shard", "seq", None),
        P("shard", None),
        P("shard", None),
        P("shard"),
        P("shard"),
        P("shard", None),
        P("shard"),
        P("shard"),
        P("shard"),
        P("shard", None),
        P("shard"),
        P("shard", None),
        P("shard"),
        P("shard"),
        P("shard"),
        P(None, "shard", "seq", None),
    )
    return jax.shard_map(
        layer,
        mesh=mesh,
        in_specs=placed,
        out_specs=(
            P(None, "shard", "seq", None),
            P(None, "shard", "seq", None),
            P("shard", None),
            P("shard"),
            P("shard"),
            P("shard", None),
            P("shard"),
            P("shard"),
            P("shard"),
            P("shard", None),
            P("shard"),
            P("shard", None),
            P("shard"),
            P("shard"),
            P("shard"),
        ),
        check_vma=False,
    )
```
